32 devices in a mesh: dp: 8 (over z, y), expert: 2 (over x), tensor: 2 (over core).
Axes of the slice: x: 2, y: 2, z: 4, core: 2. Of those that a mesh axis runs over, the one named last changes fastest.
Arguments:
- tokens: bfloat16 [512, 4096], P('dp', 'tensor'), may hold values from -6 to 6
- targets: bfloat16 [512, 4096], P('dp', 'tensor'), may hold values from -6 to 6
- norm_gain: float32 [4096], P('tensor'), may hold values from 0.1 to 1.9
- expert_ids: int32 [512, 2], P('dp'), may hold values from 0 to 7, all different within a row; in each aligned block of 64 rows (0 to 63, 64 to 127, ...) at most 18 rows name the same one
- gate_prob: float32 [512, 2], P('dp'), may hold values from 0.2 to 1
- w_gate: bfloat16 [4096, 65536], P('tensor', ('dp', 'expert')), may hold values from -0.09375 to 0.09375
- gate_probe: bfloat16 [4096, 65536], P('tensor', ('dp', 'expert')), as said below
- w_up: bfloat16 [4096, 65536], P('tensor', ('dp', 'expert')), may hold values from -0.09375 to 0.09375
- w_down: bfloat16 [65536, 4096], P(('dp', 'expert'), 'tensor'), may hold values from -0.0625 to 0.0625
Outputs:
- normed: bfloat16 [512, 4096], P('dp', 'tensor')
- curvature: float32 [512, 2], P('dp')
- estimate: float32 [8], replicated
The draws below stay inside these ranges and needn't reach their ends.
Inputs may be any that keep to these rules, and one draw needn't show every extreme that they name: `expert_ids`: the two ids of a token differ; within each block of 64 consecutive tokens no expert is named more than 18 times; every expert is named by some token. `gate_probe`: every entry is plus or minus 1 / sqrt(4096).
All inputs are finite; a program needn't handle non-finite values.
Results may differ from the reference program's by a relative error of at most 0.03.
Values may be sent and summed in bfloat16 or wider, within the bound.
No kernel may reach another device: no remote copies, remote signals or barrier semaphores. Data moves between devices by JAX's collectives and lax.ppermute only.
A program may use at most 128 MiB of HBM per device.

```python
import math
import jax
import jax.numpy as jnp
import numpy as np
from jax import lax

D = 4096
FF = 8192
EXPERTS = 8
TOK_DEV = 64
CAP = 18
TOKENS = 512
N_DP = 8
N_EXPERT = 2
N_TENSOR = 2


def draw_gate_probe(key, part):
    signs = jax.random.bernoulli(key, 0.5, (D, EXPERTS * FF))
    values = jnp.where(signs, 1.0, -1.0).astype(jnp.float32) * D ** (-0.5)
    return values.astype(jnp.bfloat16)


def block_levels(own_key, extent, cuts, low, largest):
    factor_of = 1.0
    for position, parts in cuts:
        heights = jax.random.uniform(jax.random.fold_in(jax.random.fold_in(own_key, 6), position), (parts,), jnp.float32, low / len(cuts), largest / len(cuts))
        factor_of = factor_of * jnp.repeat(jnp.exp(heights), extent[position] // parts).reshape((-1,) + (1,) * (len(extent) - 1 - position))
    return factor_of


def deal_out(key, own, number, rows, amount, top, bound, lean):
    sequence = jax.random.permutation(key, amount)
    packed, common = load_shares(amount, rows * top, bound, lean, True), load_shares(amount, rows * top, bound, lean, False)
    places = jnp.arange(amount)

    def named(lengths, rotation):
        used = int((lengths > 0).sum())
        fixed = max(1, used // 4)
        passed = fixed + (places - fixed + rotation * (used - fixed)) % max(1, amount - fixed)
        return jnp.zeros((amount,), jnp.int32).at[sequence[jnp.where(places < fixed, places, passed)]].set(jnp.asarray(lengths, jnp.int32))

    lengths = jnp.where(number % 4 == 0, named(packed, number // 4), named(common, number - number // 4 - 1))
    mixed = jax.random.permutation(jax.random.fold_in(own, 3), amount)
    donor, taker = mixed[0:amount // 2 * 2:2], mixed[1:amount // 2 * 2:2]
    margin = jnp.minimum(lengths[donor] - 1, bound - lengths[taker]) // 2
    margin = jnp.where((donor == sequence[0]) | (taker == sequence[0]) | (lengths[taker] == 0), 0, jnp.maximum(margin, 0))
    passed = jax.random.randint(jax.random.fold_in(own, 4), (amount // 2,), 0, 1 << 20) % (margin + 1)
    lengths = lengths.at[donor].add(-passed).at[taker].add(passed)
    items = jnp.searchsorted(jnp.cumsum(lengths), jnp.arange(rows * top), side="right").astype(jnp.int32)
    listing = items.reshape(top, rows).T
    listing = listing[jax.random.permutation(jax.random.fold_in(own, 1), rows)]
    rotation = jax.random.randint(jax.random.fold_in(own, 2), (rows, 1), 0, top)
    return jnp.take_along_axis(listing, (jnp.arange(top)[None, :] + rotation) % top, axis=1)


def load_shares(number_of, total, limit, lean, full):
    loads = [(1 << 20) // math.isqrt(grade ** lean) + 1 for grade in range(1, number_of + 1)]
    largest = limit if full else min(limit, max(-(-total // number_of), total * loads[0] // sum(loads)))
    least = 1 if total - largest >= number_of - 1 else 0
    given, rest = [largest] + [least] * (number_of - 1), total - largest - least * (number_of - 1)
    while rest > 0:
        free = [i for i in range(1, number_of) if given[i] < largest] or [i for i in range(1, number_of) if given[i] < limit]
        whole, left = sum([loads[i] for i in free]), rest
        for i in free:
            addition = min(limit - given[i], max(1, left * loads[i] // whole), rest)
            given[i] = given[i] + addition
            rest = rest - addition
    return np.array(given)


def gaussian(key, extent, scale, most, shards=(), kind=jnp.bfloat16):
    level = block_levels(key, extent, shards, -0.22, 0.18) if shards else 1.0
    drawn = jax.random.normal(key, extent, jnp.float32) * scale * level
    return jnp.minimum(jnp.maximum(drawn, -most), most).astype(kind)


def setup_inputs(seed: int = 0) -> dict:
    key_of = jax.random.split(jax.random.key(seed), 10)
    tokens = gaussian(key_of[0], (TOKENS, D), 1.0, 6.0, ((0, 8), (1, 2)))
    targets = gaussian(key_of[1], (TOKENS, D), 1.0, 6.0, ((0, 8), (1, 2)))
    norm_gain = jnp.clip(1.0 + 0.18 * jax.random.normal(key_of[2], (D,), jnp.float32), 0.1, 1.9)
    expert_ids_keys = jax.random.split(jax.random.fold_in(key_of[3], 1), TOKENS // TOK_DEV)
    expert_ids_turns = jax.random.permutation(jax.random.fold_in(key_of[3], 3), TOKENS // TOK_DEV)
    expert_ids = jax.vmap(lambda own, number: deal_out(jax.random.fold_in(key_of[3], 2), own, number, TOK_DEV, EXPERTS, 2, CAP, 2))(expert_ids_keys, expert_ids_turns).reshape((TOKENS, 2))
    gate_prob = jnp.clip(0.2 + 0.8 * jax.random.uniform(key_of[4], (TOKENS, 2), jnp.float32) ** block_levels(key_of[4], (TOKENS, 2), ((0, 8),), -0.2, 0.2), 0.2, 1.0)
    w_gate = gaussian(key_of[5], (D, EXPERTS * FF), D ** -0.5, 0.09375, ((0, 2), (1, 16)))
    gate_probe = draw_gate_probe(jax.random.fold_in(key_of[9], 71), 0)
    w_up = gaussian(key_of[7], (D, EXPERTS * FF), D ** -0.5, 0.09375, ((0, 2), (1, 16)))
    w_down = gaussian(key_of[8], (EXPERTS * FF, D), FF ** -0.5, 0.0625, ((0, 16), (1, 2)))
    return {"tokens": tokens, "targets": targets, "norm_gain": norm_gain, "expert_ids": expert_ids, "gate_prob": gate_prob, "w_gate": w_gate, "gate_probe": gate_probe, "w_up": w_up, "w_down": w_down}


epsilon = 1e-05
loss_weight = 8.0

def derivative_jets(preact):
    gate_in = preact[:, 0]
    gate_dir = preact[:, 1]
    up_in = preact[:, 2]
    sigmoid_in = jax.nn.sigmoid(gate_in)
    first_slope = sigmoid_in * (1.0 + gate_in * (1.0 - sigmoid_in))
    second_slope = sigmoid_in * (1.0 - sigmoid_in) * (2.0 + gate_in * (1.0 - 2.0 * sigmoid_in))
    primal = gate_in * sigmoid_in * up_in
    tangent = first_slope * gate_dir * up_in
    second = second_slope * gate_dir * gate_dir * up_in
    return jnp.stack([primal, tangent, second], axis=1).astype(jnp.bfloat16)

def slot_numbers(expert_ids):
    blocks = expert_ids.reshape(N_DP, TOK_DEV * 2)
    onehot = (blocks[:, :, None] == jnp.arange(EXPERTS, dtype=jnp.int32)).astype(jnp.int32)
    before = jnp.cumsum(onehot, axis=1).astype(jnp.int32) - onehot
    return lax.optimization_barrier(jnp.sum(before * onehot, axis=2)).astype(jnp.int32).reshape(TOKENS, 2)

def blocked_sum(left_blocks, right_blocks):
    partial_value = jnp.einsum('rbi,bic->rbc', left_blocks, right_blocks)
    rounded = lax.optimization_barrier(partial_value.astype(jnp.bfloat16))
    return lax.optimization_barrier(jnp.sum(rounded.astype(jnp.float32), axis=1))

def reference(tokens, targets, norm_gain, expert_ids, gate_prob, w_gate, gate_probe, w_up, w_down):
    slot_rows = N_DP * CAP
    width_part = D // N_TENSOR
    pieces = N_DP * N_EXPERT // EXPERTS
    hidden_part = FF // pieces
    slot_index = slot_numbers(expert_ids)
    owner_index = (jnp.arange(TOKENS, dtype=jnp.int32) // TOK_DEV).astype(jnp.int32)[:, None]
    places = ((expert_ids * N_DP + owner_index) * CAP + slot_index).reshape(-1).astype(jnp.int32)
    dispatched = jnp.zeros((EXPERTS * slot_rows, D), jnp.bfloat16).at[places].set(jnp.repeat(tokens, 2, axis=0))
    dispatched = dispatched.reshape(EXPERTS, slot_rows, D)

    def expert_images(carried):
        expert_index, expert_rows = carried
        split_rows = expert_rows.astype(jnp.float32).reshape(slot_rows, N_TENSOR, width_part)

        def preact_of(weight):
            weight_cols = lax.dynamic_slice_in_dim(weight, expert_index * FF, FF, 1)
            return blocked_sum(split_rows, weight_cols.astype(jnp.float32).reshape(N_TENSOR, width_part, FF))
        hidden_jets = derivative_jets(jnp.stack([preact_of(w_gate), preact_of(gate_probe), preact_of(w_up)], axis=1))
        down_rows = lax.dynamic_slice_in_dim(w_down, expert_index * FF, FF, 0)
        down_rows = down_rows.astype(jnp.float32).reshape(pieces, hidden_part, D)
        images = blocked_sum(hidden_jets.astype(jnp.float32).reshape(slot_rows * 3, pieces, hidden_part), down_rows)
        return images.reshape(slot_rows, 3, D)
    expert_table = lax.map(expert_images, (jnp.arange(EXPERTS, dtype=jnp.int32), dispatched))
    picked = expert_table.reshape(EXPERTS * slot_rows, 3, D)[places].reshape(TOKENS, 2, 3, D)
    weights = gate_prob[:, :, None]
    summed = tokens.astype(jnp.float32) + lax.optimization_barrier(jnp.sum(weights * picked[:, :, 0], axis=1))
    tangent_out = weights * picked[:, :, 1]
    second_out = weights * picked[:, :, 2]
    target = targets.astype(jnp.float32)
    inv_root = lax.rsqrt(lax.optimization_barrier(jnp.mean(summed * summed, axis=-1)) + epsilon)
    normed = (norm_gain * summed * inv_root[:, None]).astype(jnp.bfloat16)

    def slot_loss(travel):
        shifted = summed[:, None, :] + travel[:, :, None] * tangent_out + 0.5 * (travel * travel)[:, :, None] * second_out
        inv_scale = lax.rsqrt(lax.optimization_barrier(jnp.mean(shifted * shifted, axis=-1)) + epsilon)
        misfit = norm_gain * shifted * inv_scale[:, :, None] - target[:, None, :]
        return loss_weight / D * lax.optimization_barrier(jnp.sum(misfit * misfit, axis=-1))
    unit_step = jnp.ones((TOKENS, 2), jnp.float32)

    def slope_at(travel):
        return jax.jvp(slot_loss, (travel,), (unit_step,))[1]
    curvature = jax.jvp(slope_at, (jnp.zeros((TOKENS, 2), jnp.float32),), (unit_step,))[1]
    member = (expert_ids[:, :, None] == jnp.arange(EXPERTS, dtype=jnp.int32)).astype(jnp.float32)
    totals = lax.optimization_barrier(jnp.sum(member * curvature[:, :, None], axis=(0, 1)))
    counts = lax.optimization_barrier(jnp.sum(member, axis=(0, 1)))
    return (normed, curvature, totals / counts)
```

```python
import functools

import jax
import jax.numpy as jnp
from jax import lax
from jax.experimental import pallas as pl
from jax.experimental.pallas import tpu as pltpu
from jax.sharding import PartitionSpec as P


D = 4096
EXPERTS = 8
CAP = 18
LANE_PARTS = 4
OUT_ROWS = 56
GROUP = 4
PAIR = 2
PART_ROWS = 80
HIDDEN_CHUNKS = 4
MIB = 1024 * 1024

epsilon = 1e-05
loss_weight = 8.0
f32 = jnp.float32
bf16 = jnp.bfloat16


def in_hbm(array):
    return pltpu.with_memory_space_constraint(array, pltpu.HBM)


def in_vmem(array):
    return pltpu.with_memory_space_constraint(array, pltpu.VMEM)


def slot_rows(ids):
    count = ids.shape[1]
    line = lax.broadcasted_iota(jnp.int32, (EXPERTS, count), 0)
    rows = [ids[i : i + 1, :] for i in range(2)]
    hots = [(line == r).astype(f32) for r in rows]
    earlier = lax.broadcasted_iota(jnp.int32, (count, count), 0) < lax.broadcasted_iota(
        jnp.int32, (count, count), 1
    )
    before = jnp.dot(
        (hots[0] + hots[1]).astype(bf16), earlier.astype(bf16), preferred_element_type=f32
    )
    slots = [jnp.sum(before * h, axis=0, keepdims=True).astype(jnp.int32) for h in hots]
    return rows, hots, slots


def upright(row):
    count = row.shape[1]
    same = lax.broadcasted_iota(jnp.int32, (count, count), 0) == lax.broadcasted_iota(
        jnp.int32, (count, count), 1
    )
    return jnp.sum(jnp.where(same, row, jnp.zeros_like(row)), axis=1, keepdims=True)


def dispatch_body(where_ref, ids_ref, tokens_hbm, *refs):
    outs, (tokens_ref, sem) = refs[:EXPERTS], refs[EXPERTS:]
    fetch = pltpu.make_async_copy(tokens_hbm, tokens_ref, sem)
    fetch.start()
    rows, _, slots = slot_rows(ids_ref[...])
    block = LANE_PARTS * CAP
    line = lax.broadcasted_iota(jnp.int32, (EXPERTS * block, ids_ref.shape[1]), 0)
    firsts = [(r ^ where_ref[1]) * block + s for r, s in zip(rows, slots)]
    selects = []
    for q in range(LANE_PARTS):
        hit = [line == first + q * CAP for first in firsts]
        selects.append((hit[0] | hit[1]).astype(f32).astype(bf16))
    lanes = outs[0].shape[1]
    fetch.wait()
    out = None
    for q in range(LANE_PARTS):
        term = jnp.dot(
            selects[q], tokens_ref[:, q * lanes : (q + 1) * lanes], preferred_element_type=f32
        )
        out = term if out is None else out + term
    for j in range(EXPERTS):
        outs[j][...] = out[j * block : (j + 1) * block].astype(bf16)


def dispatch(where, ids_t, tokens):
    rows, width = tokens.shape
    vmem = pl.BlockSpec(memory_space=pltpu.VMEM)
    return pl.pallas_call(
        dispatch_body,
        out_shape=[jax.ShapeDtypeStruct((LANE_PARTS * CAP, width // LANE_PARTS), bf16)] * EXPERTS,
        in_specs=[pl.BlockSpec(memory_space=pltpu.SMEM), vmem, pl.BlockSpec(memory_space=pltpu.HBM)],
        out_specs=[vmem] * EXPERTS,
        scratch_shapes=[pltpu.VMEM((rows, width), bf16), pltpu.SemaphoreType.DMA],
        compiler_params=pltpu.CompilerParams(vmem_limit_bytes=8 * MIB),
        name="dispatch",
    )(where, ids_t, in_hbm(tokens))


def fetch_body(*refs):
    count = (len(refs) - 1) // 2
    sems = refs[-1]
    copies = [
        pltpu.make_async_copy(refs[i], refs[count + i], sems.at[i]) for i in range(count)
    ]
    for copy in copies:
        copy.start()
    for copy in copies:
        copy.wait()


def fetch(*arrays):
    return pl.pallas_call(
        fetch_body,
        out_shape=[pltpu.VMEM(a.shape, a.dtype) for a in arrays],
        in_specs=[pl.BlockSpec(memory_space=pltpu.HBM)] * len(arrays),
        out_specs=[pl.BlockSpec(memory_space=pltpu.VMEM)] * len(arrays),
        scratch_shapes=[pltpu.SemaphoreType.DMA((len(arrays),))],
        compiler_params=pltpu.CompilerParams(vmem_limit_bytes=MIB),
        cost_estimate=pl.CostEstimate(
            flops=3 * 10**9 * len(arrays), bytes_accessed=sum(2 * a.size for a in arrays), transcendentals=0
        ),
        name="fetch",
    )(*[in_hbm(a) for a in arrays])


def preact_body(first, count, *refs):
    blocks = refs[:count]
    near_ref, *far, out_ref, rows_ref, held_ref, sems = refs[count:]
    size = out_ref.shape[2]
    steps = sems.shape[1]
    tile = size // steps
    copies = [
        [
            pltpu.make_async_copy(
                hbm.at[:, pl.ds(first + t * tile, tile)],
                held_ref.at[w, :, pl.ds(t * tile, tile)],
                sems.at[w, t],
            )
            for t in range(steps)
        ]
        for w, hbm in enumerate(far)
    ]
    for copy in sum(copies, []):
        copy.start()
    lanes = blocks[0].shape[1]
    tail = jnp.zeros((PART_ROWS - GROUP * CAP, lanes), f32)
    for g in range(count // GROUP):
        mine = [blocks[g * GROUP + i][...].astype(f32) for i in range(GROUP)]
        for q in range(LANE_PARTS):
            rows_ref[g * PART_ROWS : (g + 1) * PART_ROWS, q * lanes : (q + 1) * lanes] = (
                jnp.concatenate([b[q * CAP : (q + 1) * CAP] for b in mine] + [tail], axis=0)
            ).astype(bf16)
    rows = rows_ref[...]
    for part in range(3):
        for t in range(steps):
            if part:
                copies[part - 1][t].wait()
                weight = held_ref[part - 1, :, t * tile : (t + 1) * tile]
            else:
                weight = near_ref[:, first + t * tile : first + (t + 1) * tile]
            out_ref[part, :, t * tile : (t + 1) * tile] = jnp.dot(
                rows, weight, preferred_element_type=f32
            ).astype(bf16)


def preact(arrived, near, far, chunk, size):
    count = len(arrived)
    width = near.shape[0]
    total = count // GROUP * PART_ROWS
    vmem = pl.BlockSpec(memory_space=pltpu.VMEM)
    steps = max(1, size // 256)
    return pl.pallas_call(
        functools.partial(preact_body, chunk * size, count),
        out_shape=jax.ShapeDtypeStruct((3, total, size), bf16),
        in_specs=[vmem] * (count + 1) + [pl.BlockSpec(memory_space=pltpu.HBM)] * 2,
        out_specs=vmem,
        scratch_shapes=[
            pltpu.VMEM((total, width), bf16),
            pltpu.VMEM((2, width, size), bf16),
            pltpu.SemaphoreType.DMA((2, steps)),
        ],
        compiler_params=pltpu.CompilerParams(vmem_limit_bytes=16 * MIB),
        cost_estimate=pl.CostEstimate(
            flops=6 * total * width * size, bytes_accessed=6 * width * size, transcendentals=0
        ),
        name="preact",
    )(*arrived, in_vmem(near), *[in_hbm(w) for w in far])


def jets_body(first, own_ref, peer_ref, down_hbm, *refs):
    outs = refs[:-2]
    down_ref, sem = refs[-2:]
    copy = pltpu.make_async_copy(down_hbm.at[pl.ds(first, down_ref.shape[0])], down_ref, sem)
    copy.start()
    size = own_ref.shape[2]
    tile = min(512, size)
    for g, out in enumerate(outs):

        @pl.loop(0, PART_ROWS // 16)
        def _(step):
            at = pl.multiple_of(step * 16, 16)
            for t in range(size // tile):
                lane = pl.ds(t * tile, tile)
                place = (pl.ds(g * PART_ROWS + at, 16), lane)
                gate_in, gate_dir, up_in = (
                    own_ref[(i,) + place].astype(f32) + peer_ref[(i,) + place].astype(f32)
                    for i in range(3)
                )
                turn = jnp.tanh(0.5 * gate_in)
                sig = 0.5 + 0.5 * turn
                rest = 0.5 - 0.5 * turn
                first_slope = sig * (1.0 + gate_in * rest)
                second_slope = (sig * rest) * (2.0 - gate_in * turn)
                along = gate_dir * up_in
                parts = (
                    (gate_in * sig) * up_in,
                    first_slope * along,
                    second_slope * (gate_dir * along),
                )
                for i, part in enumerate(parts):
                    out[i, pl.ds(at, 16), lane] = part.astype(bf16)

    copy.wait()


def jets(own, peer, w_down, chunk, groups):
    _, rows, size = own.shape
    vmem = pl.BlockSpec(memory_space=pltpu.VMEM)
    return pl.pallas_call(
        functools.partial(jets_body, chunk * size),
        out_shape=[jax.ShapeDtypeStruct((3, PART_ROWS, size), bf16)] * groups
        + [pltpu.VMEM((size, w_down.shape[1]), bf16)],
        in_specs=[vmem, vmem, pl.BlockSpec(memory_space=pltpu.HBM)],
        out_specs=[vmem] * (groups + 1),
        scratch_shapes=[pltpu.SemaphoreType.DMA],
        compiler_params=pltpu.CompilerParams(vmem_limit_bytes=8 * MIB),
        cost_estimate=pl.CostEstimate(
            flops=40 * 3 * rows * size, bytes_accessed=18 * rows * size, transcendentals=rows * size
        ),
        name="jets",
    )(own, peer, in_hbm(w_down))


def images_body(chunks, other, where_ref, *refs):
    hidden = refs[:chunks]
    down = refs[chunks : 2 * chunks]
    outs = refs[2 * chunks :]
    size = hidden[0].shape[2]
    width = outs[0].shape[2]
    tile = min(256, width)
    half = 1 - where_ref[0] if other else where_ref[0]
    for t in range(width // tile):
        lanes = pl.ds(pl.multiple_of(half * width + t * tile, tile), tile)
        acc = None
        for c in range(chunks):
            left = hidden[c][...].reshape(3 * PART_ROWS, size)
            term = jnp.dot(left, down[c][:, lanes], preferred_element_type=f32)
            acc = term if acc is None else acc + term
        tail = jnp.zeros((OUT_ROWS - 3 * CAP, tile), f32)
        for i in range(GROUP):
            first = [p * PART_ROWS + i * CAP for p in range(3)]
            outs[i // PAIR][i % PAIR, :, t * tile : (t + 1) * tile] = jnp.concatenate(
                [acc[r : r + CAP] for r in first] + [tail], axis=0
            ).astype(bf16)


def images(where, other, hidden, down):
    chunks = len(hidden)
    size = hidden[0].shape[2]
    width = down[0].shape[1] // 2
    vmem = pl.BlockSpec(memory_space=pltpu.VMEM)
    return pl.pallas_call(
        functools.partial(images_body, chunks, other),
        in_specs=[pl.BlockSpec(memory_space=pltpu.SMEM)] + [vmem] * (2 * chunks),
        out_specs=[vmem] * (GROUP // PAIR),
        out_shape=[jax.ShapeDtypeStruct((PAIR, OUT_ROWS, width), bf16)] * (GROUP // PAIR),
        compiler_params=pltpu.CompilerParams(vmem_limit_bytes=8 * MIB),
        cost_estimate=pl.CostEstimate(
            flops=6 * GROUP * CAP * chunks * size * width,
            bytes_accessed=2 * chunks * size * width,
            transcendentals=0,
        ),
        name="images",
    )(where, *hidden, *[in_vmem(d) for d in down])


def moments_body(count, where_ref, ids_ref, prob_ref, tokens_ref, targets_ref, gain_ref, *refs):
    blocks = refs[:count]
    stats_ref, summed_ref, sent_ref = refs[count:]
    holders = count // EXPERTS
    mine = where_ref[1]
    ids, _, slots = slot_rows(ids_ref[...])
    rows = ids[0].shape[1]
    starts = [upright((r ^ mine) * (holders * OUT_ROWS) + s) for r, s in zip(ids, slots)]
    table = jnp.concatenate([b[...].astype(f32) for b in blocks], axis=0).astype(bf16)
    lanes = lax.broadcasted_iota(jnp.int32, (rows, count * OUT_ROWS), 1)
    pieces = []
    for part in range(3):
        for i in range(2):
            hit = None
            for j in range(holders):
                same = lanes == starts[i] + (j * OUT_ROWS + part * CAP)
                hit = same if hit is None else hit | same
            pieces.append(hit.astype(f32))
    select = jnp.concatenate(pieces, axis=0).astype(bf16)
    picked = jnp.dot(select, table, preferred_element_type=f32)
    probs = [upright(prob_ref[i : i + 1, :]) for i in range(2)]
    part_of = lambda part, i: picked[(2 * part + i) * rows : (2 * part + i + 1) * rows] * probs[i]
    summed = tokens_ref[...].astype(f32) + (part_of(0, 0) + part_of(0, 1))
    summed_ref[...] = summed
    gain = gain_ref[...]
    sent_ref[...] = (gain * summed).astype(bf16)
    weighted = gain * gain * summed
    aim = gain * targets_ref[...].astype(f32)
    total = lambda v: jnp.sum(v, axis=1, keepdims=True)
    columns = [total(summed * summed), total(weighted * summed), total(aim * summed)]
    for i in range(2):
        along, bend = part_of(1, i), part_of(2, i)
        columns += [
            total(summed * along),
            total(along * along),
            total(summed * bend),
            total(gain * gain * along * along),
            total(weighted * along),
            total(weighted * bend),
            total(aim * along),
            total(aim * bend),
        ]
    place = lax.broadcasted_iota(jnp.int32, (rows, 128), 1)
    stats = jnp.zeros((rows, 128), f32)
    for c, column in enumerate(columns):
        stats = jnp.where(place == c, column, stats)
    stats_ref[...] = stats


def moments(where, ids_t, prob_t, tokens, targets, gain, blocks):
    count = len(blocks)
    rows = tokens.shape[0]
    half = tokens.shape[1] // 2
    whole = lambda shape: pl.BlockSpec(shape, lambda i, w: (0,) * len(shape))
    split = lambda r: pl.BlockSpec((r, half), lambda i, w: (0, w[0]))
    return pl.pallas_call(
        functools.partial(moments_body, count),
        grid_spec=pltpu.PrefetchScalarGridSpec(
            num_scalar_prefetch=1,
            grid=(1,),
            in_specs=[whole((2, rows)), whole((2, rows)), split(rows), split(rows), split(1)]
            + [whole((OUT_ROWS, half))] * count,
            out_specs=[whole((rows, 128)), whole((rows, half)), whole((rows, half))],
        ),
        out_shape=[
            jax.ShapeDtypeStruct((rows, 128), f32),
            jax.ShapeDtypeStruct((rows, half), f32),
            jax.ShapeDtypeStruct((rows, half), bf16),
        ],
        compiler_params=pltpu.CompilerParams(vmem_limit_bytes=40 * MIB),
        cost_estimate=pl.CostEstimate(
            flops=12 * rows * count * OUT_ROWS * half, bytes_accessed=MIB, transcendentals=0
        ),
        name="moments",
    )(where, ids_t, prob_t, tokens, targets, gain, *blocks)


def curve_body(
    where_ref, ids_ref, stats_ref, more_ref, summed_ref, gain_ref, other_ref, *outs
):
    normed_ref, curve_ref, sums_ref = outs
    stats = stats_ref[...] + more_ref[...]
    rows = stats.shape[0]
    col = lambda c: stats[:, c : c + 1]
    inv_root = lax.rsqrt(col(0) / D + epsilon)
    side = where_ref[0]
    width = summed_ref.shape[1]
    near = pl.ds(pl.multiple_of(side * width, width), width)
    far = pl.ds(pl.multiple_of((1 - side) * width, width), width)
    normed_ref[:, near] = (gain_ref[...] * summed_ref[...] * inv_root).astype(bf16)
    normed_ref[:, far] = (other_ref[...].astype(f32) * inv_root).astype(bf16)
    weighted_uu = col(1)
    resid_u = inv_root * weighted_uu - col(2)
    inv_cube = inv_root * inv_root * inv_root
    lanes = lax.broadcasted_iota(jnp.int32, (rows, 128), 1)
    totals = jnp.zeros((rows, 128), f32)
    counts = jnp.zeros((rows, 128), f32)
    for i in range(2):
        ua, aa, ub, waa, wau, wub, ta, tb = (col(3 + 8 * i + j) for j in range(8))
        resid_a = inv_root * wau - ta
        resid_b = inv_root * wub - tb
        first_rate = 2.0 * ua / D
        second_rate = 2.0 * (aa + ub) / D
        slope_one = -0.5 * inv_cube * first_rate
        slope_two = (
            0.75 * inv_cube * inv_root * inv_root * first_rate * first_rate
            - 0.5 * inv_cube * second_rate
        )
        tangent_sq = (
            inv_root * inv_root * waa
            + 2.0 * inv_root * slope_one * wau
            + slope_one * slope_one * weighted_uu
        )
        bending = inv_root * resid_b + 2.0 * slope_one * resid_a + slope_two * resid_u
        curvature = 2.0 * loss_weight / D * (tangent_sq + bending)
        curve_ref[:, i : i + 1] = curvature
        member = (lanes == upright(ids_ref[i : i + 1, :])).astype(f32)
        totals = totals + member * curvature
        counts = counts + member
    line = lax.broadcasted_iota(jnp.int32, (8, 128), 0)
    sums_ref[...] = jnp.where(
        line == 0,
        jnp.sum(totals, axis=0, keepdims=True),
        jnp.where(line == 1, jnp.sum(counts, axis=0, keepdims=True), 0.0),
    )


def curve(where, ids_t, stats, more, summed, gain, other):
    rows, half = summed.shape
    whole = lambda shape: pl.BlockSpec(shape, lambda i, w: (0,) * len(shape))
    return pl.pallas_call(
        curve_body,
        grid_spec=pltpu.PrefetchScalarGridSpec(
            num_scalar_prefetch=1,
            grid=(1,),
            in_specs=[
                whole((2, rows)),
                whole((rows, 128)),
                whole((rows, 128)),
                whole((rows, half)),
                pl.BlockSpec((1, half), lambda i, w: (0, w[0])),
                whole((rows, half)),
            ],
            out_specs=[whole((rows, 2 * half)), whole((rows, 2)), whole((8, 128))],
        ),
        out_shape=[
            jax.ShapeDtypeStruct((rows, 2 * half), bf16),
            jax.ShapeDtypeStruct((rows, 2), f32),
            jax.ShapeDtypeStruct((8, 128), f32),
        ],
        compiler_params=pltpu.CompilerParams(vmem_limit_bytes=12 * MIB),
        name="curve",
    )(where, ids_t, stats, more, summed, gain, other)


def swap(value, axis, mask=1):
    n = lax.axis_size(axis)
    return lax.ppermute(value, axis, [(i, i ^ mask) for i in range(n)])


def layer(tokens, targets, norm_gain, expert_ids, gate_prob, w_gate, gate_probe, w_up, w_down):
    n = lax.axis_size("dp")
    holders = n // EXPERTS
    hidden_part = w_gate.shape[1]
    where = jnp.stack([lax.axis_index("expert"), lax.axis_index("dp") // holders]).astype(jnp.int32)
    gain = norm_gain.reshape(1, -1)
    ids_t, prob_t = expert_ids.T, gate_prob.T

    outgoing = dispatch(where, ids_t, tokens)
    arrived = [outgoing[0]] * n
    for k in range(1, n):
        arrived[k] = swap(outgoing[k // holders], "dp", k)
    (near_gate,) = fetch(w_gate)

    size = hidden_part // HIDDEN_CHUNKS
    groups = n // GROUP
    hidden = [[] for _ in range(groups)]
    down = []
    for c in range(HIDDEN_CHUNKS):
        own = preact(arrived, near_gate, (gate_probe, w_up), c, size)
        *parts, rows = jets(own, swap(own, "tensor"), w_down, c, groups)
        down.append(rows)
        for g, part in enumerate(parts):
            hidden[g].append(part)

    returned = [None] * n
    for g in range(groups - 1, -1, -1):
        theirs = images(where, True, hidden[g], down)
        got = [swap(v, "expert") for v in theirs]
        ours = images(where, False, hidden[g], down)
        for i in range(GROUP - 1, -1, -1):
            k = g * GROUP + i
            pair = [v[i // PAIR][i % PAIR].astype(f32) for v in (ours, got)]
            both = (pair[0] + pair[1]).astype(bf16)
            returned[k] = swap(both, "dp", k) if k else both

    stats, summed, sent = moments(where, ids_t, prob_t, tokens, targets, gain, returned)
    other = swap(sent, "expert")
    stats = stats + swap(stats, "tensor")
    more = swap(stats, "expert")
    normed, curvature, sums = curve(where, ids_t, stats, more, summed, gain, other)
    step = n // 2
    while step:
        sums = sums + swap(sums, "dp", step)
        step //= 2
    return (normed, curvature, sums[0, :EXPERTS] / sums[1, :EXPERTS])


def solution(mesh):
    return jax.shard_map(
        layer,
        mesh=mesh,
        in_specs=(
            P("dp", "tensor"),
            P("dp", "tensor"),
            P("tensor"),
            P("dp", None),
            P("dp", None),
            P("tensor", ("dp", "expert")),
            P("tensor", ("dp", "expert")),
            P("tensor", ("dp", "expert")),
            P(("dp", "expert"), "tensor"),
        ),
        out_specs=(P("dp", "tensor"), P("dp", None), P()),
        check_vma=False,
    )
```
